16 devices in a mesh: stage: 2 (over z), data: 8 (over y, x, core).
Axes of the slice: x: 2, y: 2, z: 2, core: 2. Of those that a mesh axis runs over, the one named last changes fastest.
Arguments:
- x_in: bfloat16 [8, 512, 768], P(None, 'data')
- targets: bfloat16 [8, 512, 768], P(None, 'data')
- w_work: bfloat16 [2, 6, 4718592], P('stage')
- w_master: float32 [2, 6, 4718592], P('stage', None, 'data')
- m_prior: float32 [2, 6, 4718592], P('stage', None, 'data')
- v_prior: float32 [2, 6, 4718592], P('stage', None, 'data')
- clip_tau: float32 [], replicated
Outputs:
- output 1: float32 [], replicated
- output 2: bfloat16 [2, 6, 4718592], P('stage')
- output 3: float32 [2, 6, 4718592], P('stage', None, 'data')
- output 4: float32 [2, 6, 4718592], P('stage', None, 'data')
- output 5: float32 [2, 6, 4718592], P('stage', None, 'data')
All inputs are finite; a program needn't handle non-finite values.
Results may differ from the reference program's by a relative error of at most 0.00193934.
Values are sent between devices in bfloat16 or wider.
A program may use at most 1 GiB of HBM per device.

```python
import math
import jax
import jax.numpy as jnp
from jax import lax

D_MODEL = 768
LAYERS = 6
MICROBATCHES = 8
TOK_DEV = 64
STAGES = 2
DATA_SIZE = 8
ADAM_STEP = 10

ROW_COUNT = DATA_SIZE * TOK_DEV
HALF_LEN = 4 * D_MODEL * D_MODEL
FLAT_LEN = 2 * HALF_LEN
ADAM_BETA1 = 0.9
ADAM_BETA2 = 0.95
ADAM_EPS = 1e-8
WEIGHT_DECAY = 0.1
LEARN_RATE = 0.05 / math.sqrt(D_MODEL)


def gelu_tanh(z_val):
    return jax.nn.gelu(z_val, approximate=True)


def split_layer(w_flat):
    return w_flat[:HALF_LEN].reshape(D_MODEL, 4 * D_MODEL), w_flat[HALF_LEN:].reshape(4 * D_MODEL, D_MODEL)


def layer_forward(hidden, w_flat):
    w_in, w_out = split_layer(w_flat)
    pre_act = jnp.dot(hidden, w_in, preferred_element_type=jnp.float32).astype(jnp.bfloat16)
    act_bf = gelu_tanh(pre_act.astype(jnp.float32)).astype(jnp.bfloat16)
    out_rows = (hidden.astype(jnp.float32) + jnp.dot(act_bf, w_out, preferred_element_type=jnp.float32)).astype(jnp.bfloat16)
    return out_rows, pre_act


def layer_backward(hidden, pre_act, grad_h, w_flat):
    w_in, w_out = split_layer(w_flat)
    act_f, gelu_pull = jax.vjp(gelu_tanh, pre_act.astype(jnp.float32))
    act_bf = act_f.astype(jnp.bfloat16)
    grad_act = jnp.dot(grad_h, w_out.T, preferred_element_type=jnp.float32)
    grad_pre = gelu_pull(grad_act)[0].astype(jnp.bfloat16)
    grad_in = (grad_h.astype(jnp.float32) + jnp.dot(grad_pre, w_in.T, preferred_element_type=jnp.float32)).astype(jnp.bfloat16)
    g_first = jnp.dot(hidden.T, grad_pre, preferred_element_type=jnp.float32)
    g_second = jnp.dot(act_bf.T, grad_h, preferred_element_type=jnp.float32)
    return grad_in, jnp.concatenate([g_first.reshape(-1), g_second.reshape(-1)])


def loss_and_grads(x_in, targets, w_work):
    w_layers = w_work.reshape(-1, w_work.shape[-1])
    token_count = x_in.shape[0] * x_in.shape[1]

    def fwd_body(hidden, w_flat):
        out_rows, pre_act = layer_forward(hidden, w_flat)
        return out_rows, (hidden, pre_act)

    def bwd_body(grad_h, layer_data):
        hidden, pre_act, w_flat = layer_data
        return layer_backward(hidden, pre_act, grad_h, w_flat)

    def micro_step(scan_state, micro_batch):
        grad_acc, loss_acc = scan_state
        x_rows, t_rows = micro_batch
        y_rows, saved_acts = lax.scan(fwd_body, x_rows, w_layers)
        residual = y_rows.astype(jnp.float32) - t_rows.astype(jnp.float32)
        loss_acc = loss_acc + 0.5 * jnp.sum(residual * residual)
        grad_top = (residual / token_count).astype(jnp.bfloat16)
        _, layer_grads = lax.scan(bwd_body, grad_top, (saved_acts[0], saved_acts[1], w_layers), reverse=True)
        return (grad_acc + layer_grads, loss_acc), None

    start_state = (jnp.zeros(w_layers.shape, jnp.float32), jnp.zeros((), jnp.float32))
    (grad_acc, loss_acc), _ = lax.scan(micro_step, start_state, (x_in, targets))
    return loss_acc / token_count, grad_acc.reshape(w_work.shape)


def setup_inputs(seed: int = 0) -> dict:
    root_key = jax.random.key(seed)
    sub_keys = jax.random.split(root_key, 7)
    depth_n = STAGES * LAYERS
    x_in = jax.random.normal(sub_keys[0], (MICROBATCHES, ROW_COUNT, D_MODEL), jnp.float32).astype(jnp.bfloat16)
    targets = jax.random.normal(sub_keys[1], (MICROBATCHES, ROW_COUNT, D_MODEL), jnp.float32).astype(jnp.bfloat16)
    w_first = jax.random.normal(sub_keys[2], (STAGES, LAYERS, HALF_LEN), jnp.float32) / math.sqrt(D_MODEL)
    w_second = jax.random.normal(sub_keys[3], (STAGES, LAYERS, HALF_LEN), jnp.float32) / math.sqrt(4 * D_MODEL * depth_n)
    w_master = jnp.concatenate([w_first, w_second], axis=-1)
    w_work = w_master.astype(jnp.bfloat16)
    _, grads = loss_and_grads(x_in, targets, w_work)
    grad_norm = jnp.sqrt(jnp.sum(grads * grads))
    first_part = grads[:, :, :HALF_LEN]
    second_part = grads[:, :, HALF_LEN:]
    first_rms = jnp.sqrt(jnp.mean(first_part * first_part, axis=-1, keepdims=True))
    second_rms = jnp.sqrt(jnp.mean(second_part * second_part, axis=-1, keepdims=True))
    grad_scale = 0.4 * jnp.where(jnp.arange(FLAT_LEN) < HALF_LEN, first_rms, second_rms)
    m_prior = (1.0 - ADAM_BETA1) * grad_scale * jax.random.normal(sub_keys[4], w_master.shape, jnp.float32)
    v_prior = (1.0 - ADAM_BETA2) * grad_scale * grad_scale * jax.random.uniform(sub_keys[5], w_master.shape, jnp.float32, 0.5, 2.0)
    clip_tau = grad_norm * jax.random.uniform(sub_keys[6], (), jnp.float32, 0.3, 0.5)
    return {'x_in': x_in, 'targets': targets, 'w_work': w_work, 'w_master': w_master, 'm_prior': m_prior, 'v_prior': v_prior, 'clip_tau': clip_tau}


def reference(x_in, targets, w_work, w_master, m_prior, v_prior, clip_tau):
    loss_mean, grads = loss_and_grads(x_in, targets, w_work)
    grad_norm = jnp.sqrt(jnp.sum(grads * grads))
    clip_scale = jnp.minimum(1.0, clip_tau / grad_norm)
    scaled = clip_scale * grads
    m_new = ADAM_BETA1 * m_prior + (1.0 - ADAM_BETA1) * scaled
    v_new = ADAM_BETA2 * v_prior + (1.0 - ADAM_BETA2) * scaled * scaled
    m_hat = m_new / (1.0 - ADAM_BETA1 ** ADAM_STEP)
    v_hat = v_new / (1.0 - ADAM_BETA2 ** ADAM_STEP)
    w_new = w_master - LEARN_RATE * (m_hat / (jnp.sqrt(v_hat) + ADAM_EPS) + WEIGHT_DECAY * w_master)
    return (loss_mean, w_new.astype(jnp.bfloat16), w_new, m_new, v_new)
```

```python
import functools
import math

import jax
import jax.numpy as jnp
from jax import lax
from jax.experimental import pallas as pl
from jax.experimental.pallas import tpu as pltpu
from jax.sharding import PartitionSpec as P

ADAM_BETA1 = 0.9
ADAM_BETA2 = 0.95
ADAM_EPS = 1e-8
WEIGHT_DECAY = 0.1
ADAM_STEP = 10
LR_BASE = 0.05

D = 768
F = 3072
L = 6
ROWS = 512
TJ = 768
NT = F // TJ
LANES = 128
SHARD_Q = D * F // 4 // LANES
TOTAL_ROWS = 4096
CHUNKS = 6
CHUNK_Q = SHARD_Q // CHUNKS
LEARN_RATE = LR_BASE / math.sqrt(D)
GELU_K = math.sqrt(2.0 / math.pi)
GELU_C = 0.044715
VMEM_LIMIT = 60 * 1024 * 1024
MESH = pl.DeviceIdType.MESH
f32 = jnp.float32
bf16 = jnp.bfloat16


def _params(**kw):
    return pltpu.CompilerParams(vmem_limit_bytes=VMEM_LIMIT, **kw)


def _cost(flops, nbytes):
    return pl.CostEstimate(flops=int(flops), bytes_accessed=int(nbytes), transcendentals=0)


def _dot(a, b):
    return lax.dot_general(a, b, (((1,), (0,)), ((), ())), preferred_element_type=f32)


def _dot_nt(a, b):
    return lax.dot_general(a, b, (((1,), (1,)), ((), ())), preferred_element_type=f32)


def _dot_tn(a, b):
    return lax.dot_general(a, b, (((0,), (0,)), ((), ())), preferred_element_type=f32)


def _gelu(z):
    return z * (0.5 * (1.0 + jnp.tanh(GELU_K * (z + GELU_C * (z * z * z)))))


def _gelu_both(z):
    z2 = z * z
    t = jnp.tanh(GELU_K * (z + GELU_C * (z2 * z)))
    cdf = 0.5 * (1.0 + t)
    slope = cdf + (0.5 * z) * (1.0 - t * t) * (GELU_K + (3.0 * GELU_K * GELU_C) * z2)
    return z * cdf, slope


def _unpack_body(in_ref, o_ref, scr, *, cols, rows):
    nc = cols // LANES
    pitch = nc * 8 + 8

    def group(i, carry):
        for r in range(16):
            base = pl.multiple_of((i * 16 + r) * cols, LANES)
            v = in_ref[0, :, pl.ds(base, cols)].astype(f32)
            for cc in range(nc):
                scr[pl.ds(r * pitch + cc * 8, L), :] = v[:, cc * LANES:(cc + 1) * LANES]
        for l in range(L):
            for cc in range(nc):
                top = scr[pl.ds(cc * 8 + l, 8, stride=pitch), :]
                low = scr[pl.ds(8 * pitch + cc * 8 + l, 8, stride=pitch), :]
                row = pl.multiple_of(i * 16, 16)
                o_ref[l, pl.ds(row, 16), cc * LANES:(cc + 1) * LANES] = jnp.concatenate([top, low], axis=0).astype(bf16)
        return carry

    lax.fori_loop(0, rows // 16, group, 0)


def _unpack(w_work, n_rows, cols, rows, first):
    half = n_rows * cols
    steps = n_rows // rows
    skip = 0 if first else half // (rows * cols)
    return pl.pallas_call(
        functools.partial(_unpack_body, cols=cols, rows=rows),
        grid=(steps,),
        out_shape=jax.ShapeDtypeStruct((L, n_rows, cols), bf16),
        in_specs=[pl.BlockSpec((1, L, rows * cols), lambda i: (0, 0, i + skip))],
        out_specs=pl.BlockSpec((L, rows, cols), lambda i: (0, i, 0)),
        scratch_shapes=[pltpu.VMEM((16 * (cols // LANES * 8 + 8), LANES), f32)],
        compiler_params=_params(),
        cost_estimate=_cost(30e9, 2 * 2 * L * half),
        name="unpack_w1" if first else "unpack_w2",
    )(w_work)


def _fwd_body(x_ref, w1_ref, w2_ref, *rest, keep):
    if keep:
        xs_ref, us_ref, h_ref, cur, acc = rest
    else:
        h_ref, cur, acc = rest
    l = pl.program_id(0)
    t = pl.program_id(1)

    @pl.when((l == 0) & (t == 0))
    def _():
        cur[...] = x_ref[...]

    @pl.when(t == 0)
    def _():
        acc[...] = cur[...].astype(f32)
        if keep:
            xs_ref[0] = cur[...]

    u = _dot(cur[...], w1_ref[0]).astype(bf16)
    if keep:
        us_ref[0] = u
    a = _gelu(u.astype(f32)).astype(bf16)
    acc[...] += _dot(a, w2_ref[0])

    @pl.when(t == NT - 1)
    def _():
        cur[...] = acc[...].astype(bf16)

    @pl.when((t == NT - 1) & (l == L - 1))
    def _():
        h_ref[...] = acc[...].astype(bf16)


def _forward(x, w1, w2, keep):
    out_shape = [jax.ShapeDtypeStruct((ROWS, D), bf16)]
    out_specs = [pl.BlockSpec((ROWS, D), lambda l, t: (0, 0))]
    if keep:
        out_shape = [jax.ShapeDtypeStruct((L, ROWS, D), bf16), jax.ShapeDtypeStruct((L, ROWS, F), bf16)] + out_shape
        out_specs = [
            pl.BlockSpec((1, ROWS, D), lambda l, t: (l, 0, 0)),
            pl.BlockSpec((1, ROWS, TJ), lambda l, t: (l, 0, t)),
        ] + out_specs
    return pl.pallas_call(
        functools.partial(_fwd_body, keep=keep),
        grid=(L, NT),
        out_shape=out_shape,
        in_specs=[
            pl.BlockSpec((ROWS, D), lambda l, t: (0, 0)),
            pl.BlockSpec((1, D, TJ), lambda l, t: (l, 0, t)),
            pl.BlockSpec((1, TJ, D), lambda l, t: (l, t, 0)),
        ],
        out_specs=out_specs,
        scratch_shapes=[pltpu.VMEM((ROWS, D), bf16), pltpu.VMEM((ROWS, D), f32)],
        compiler_params=_params(),
        cost_estimate=_cost(4 * ROWS * D * F * L, 4 * D * F * L),
        name="forward_keep" if keep else "forward",
    )(x, w1, w2)


def _bwd_all_body(g_ref, u_ref, w1_ref, w2_ref, o_ref, cur, acc):
    l = pl.program_id(0)
    t = pl.program_id(1)

    @pl.when((l == 0) & (t == 0))
    def _():
        cur[...] = g_ref[...]

    @pl.when(t == 0)
    def _():
        acc[...] = cur[...].astype(f32)

    e = _dot_nt(cur[...], w2_ref[0])
    _, slope = _gelu_both(u_ref[0].astype(f32))
    acc[...] += _dot_nt((e * slope).astype(bf16), w1_ref[0])

    @pl.when(t == NT - 1)
    def _():
        cur[...] = acc[...].astype(bf16)

    @pl.when((t == NT - 1) & (l == L - 1))
    def _():
        o_ref[...] = acc[...].astype(bf16)


def _backward_all(g, u, w1, w2):
    return pl.pallas_call(
        _bwd_all_body,
        grid=(L, NT),
        out_shape=jax.ShapeDtypeStruct((ROWS, D), bf16),
        in_specs=[
            pl.BlockSpec((ROWS, D), lambda l, t: (0, 0)),
            pl.BlockSpec((1, ROWS, TJ), lambda l, t: (L - 1 - l, 0, t)),
            pl.BlockSpec((1, D, TJ), lambda l, t: (L - 1 - l, 0, t)),
            pl.BlockSpec((1, TJ, D), lambda l, t: (L - 1 - l, t, 0)),
        ],
        out_specs=pl.BlockSpec((ROWS, D), lambda l, t: (0, 0)),
        scratch_shapes=[pltpu.VMEM((ROWS, D), bf16), pltpu.VMEM((ROWS, D), f32)],
        compiler_params=_params(),
        cost_estimate=_cost(4 * ROWS * D * F * L, 4 * D * F * L),
        name="backward_all",
    )(g, u, w1, w2)


def _bwd_layer_body(g_ref, u_ref, w1_ref, w2_ref, du_ref, o_ref, acc):
    t = pl.program_id(0)

    @pl.when(t == 0)
    def _():
        acc[...] = g_ref[...].astype(f32)

    e = _dot_nt(g_ref[...], w2_ref[0])
    _, slope = _gelu_both(u_ref[0].astype(f32))
    du = (e * slope).astype(bf16)
    du_ref[...] = du
    acc[...] += _dot_nt(du, w1_ref[0])

    @pl.when(t == NT - 1)
    def _():
        o_ref[...] = acc[...].astype(bf16)


def _backward_layer(layer, g, u, w1, w2):
    return pl.pallas_call(
        _bwd_layer_body,
        grid=(NT,),
        out_shape=[jax.ShapeDtypeStruct((ROWS, F), bf16), jax.ShapeDtypeStruct((ROWS, D), bf16)],
        in_specs=[
            pl.BlockSpec((ROWS, D), lambda t: (0, 0)),
            pl.BlockSpec((1, ROWS, TJ), lambda t: (layer, 0, t)),
            pl.BlockSpec((1, D, TJ), lambda t: (layer, 0, t)),
            pl.BlockSpec((1, TJ, D), lambda t: (layer, t, 0)),
        ],
        out_specs=[pl.BlockSpec((ROWS, TJ), lambda t: (0, t)), pl.BlockSpec((ROWS, D), lambda t: (0, 0))],
        scratch_shapes=[pltpu.VMEM((ROWS, D), f32)],
        compiler_params=_params(),
        cost_estimate=_cost(4 * ROWS * D * F, 4 * D * F),
        name="backward_layer",
    )(g, u, w1, w2)


def _position():
    d = lax.axis_index("data")
    return d // 4, (d // 2) % 2, d % 2


def _wgrad_body(xo_ref, xf_ref, go_ref, gf_ref, uo_ref, duo_ref, w1_ref, w2_ref, keep_ref, send_ref, part, *, along_x):
    t = pl.program_id(0)
    yi, xi, ci = _position()
    uf = _dot(xf_ref[0], w1_ref[0]).astype(bf16)
    af, slope = _gelu_both(uf.astype(f32))
    af = af.astype(bf16)

    def grad_w1(first_col, n_cols, halves):
        duf = (_dot_nt(gf_ref[...], w2_ref[0]) * slope).astype(bf16)
        part[:n_cols, :] = _dot_tn(xo_ref[0, :, pl.ds(first_col, n_cols)], duo_ref[...]) + _dot_tn(
            xf_ref[0, :, pl.ds(first_col, n_cols)], duf
        )
        for half in range(halves):
            for rel, dst in ((0, keep_ref), (1, send_ref)):
                core = ci if rel == 0 else 1 - ci
                if along_x:
                    slot = yi
                else:
                    slot = (half + xi) % 2
                base = half * (D // 2) + core * (D // 4)

                def rows(rb, carry, base=base, dst=dst, slot=slot):
                    src = pl.multiple_of(base + rb * 8, 8)
                    for cc in range(TJ // LANES):
                        dst[slot, pl.ds(rb * 8 * (F // LANES) + t * (TJ // LANES) + cc, 8, stride=F // LANES), :] = part[
                            pl.ds(src, 8), cc * LANES:(cc + 1) * LANES
                        ]
                    return carry

                lax.fori_loop(0, D // 4 // 8, rows, 0)

    def grad_w2(dst, slot):
        ao = _gelu(uo_ref[0].astype(f32)).astype(bf16)
        part[...] = _dot_tn(ao, go_ref[...]) + _dot_tn(af, gf_ref[...])

        def rows(rb, carry):
            src = pl.multiple_of(rb * 8, 8)
            for cc in range(D // LANES):
                dst[slot, pl.ds(rb * 8 * (D // LANES) + cc, 8, stride=D // LANES), :] = part[
                    pl.ds(src, 8), cc * LANES:(cc + 1) * LANES
                ]
            return carry

        lax.fori_loop(0, TJ // 8, rows, 0)

    if along_x:
        grad_w1(pl.multiple_of(xi * (D // 2), LANES), D // 2, 1)

        @pl.when(t == 2 * xi + ci)
        def _():
            grad_w2(keep_ref, 1 - yi)

        @pl.when(t == 2 * xi + 1 - ci)
        def _():
            grad_w2(send_ref, 1 - yi)
    else:

        @pl.when(yi == 0)
        def _():
            grad_w1(0, D, 2)

        @pl.when((yi == 1) & (t % 2 == ci))
        def _():
            grad_w2(keep_ref, (t // 2 + xi) % 2)

        @pl.when((yi == 1) & (t % 2 != ci))
        def _():
            grad_w2(send_ref, (t // 2 + xi) % 2)


def _wgrad(layer, xs, xf, g, gf, us, du, w1, w2, along_x):
    out = jax.ShapeDtypeStruct((2, SHARD_Q, LANES), f32)
    return pl.pallas_call(
        functools.partial(_wgrad_body, along_x=along_x),
        grid=(NT,),
        out_shape=[out, out],
        in_specs=[
            pl.BlockSpec((1, ROWS, D), lambda t: (layer, 0, 0)),
            pl.BlockSpec((1, ROWS, D), lambda t: (0, 0, 0)),
            pl.BlockSpec((ROWS, D), lambda t: (0, 0)),
            pl.BlockSpec((ROWS, D), lambda t: (0, 0)),
            pl.BlockSpec((1, ROWS, TJ), lambda t: (layer, 0, t)),
            pl.BlockSpec((ROWS, TJ), lambda t: (0, t)),
            pl.BlockSpec((1, D, TJ), lambda t: (layer, 0, t)),
            pl.BlockSpec((1, TJ, D), lambda t: (layer, t, 0)),
        ],
        out_specs=[pl.BlockSpec((2, SHARD_Q, LANES), lambda t: (0, 0, 0))] * 2,
        scratch_shapes=[pltpu.VMEM((D, TJ), f32)],
        compiler_params=_params(),
        cost_estimate=_cost(8 * ROWS * D * F, 8 * D * F),
        name="wgrad_x" if along_x else "wgrad_y",
    )(xs, xf, g, gf, us, du, w1, w2)


def _allsum_body(x_ref, o_ref, buf, send_sem, recv_sem):
    s = lax.axis_index("stage")
    d = lax.axis_index("data")
    me = s * 8 + d
    barrier = pltpu.get_barrier_semaphore()
    for k in range(1, 16):
        peer = (me + k) % 16
        pl.semaphore_signal(barrier, inc=1, device_id=(peer // 8, peer % 8), device_id_type=MESH)
    pl.semaphore_wait(barrier, 15)
    copies = []
    for k in range(1, 16):
        peer = (me + k) % 16
        copy = pltpu.make_async_remote_copy(
            src_ref=x_ref,
            dst_ref=buf.at[k],
            send_sem=send_sem.at[k],
            recv_sem=recv_sem.at[k],
            device_id=(peer // 8, peer % 8),
            device_id_type=MESH,
        )
        copy.start()
        copies.append(copy)
    for copy in copies:
        copy.wait()
    buf[0] = x_ref[...]
    total = jnp.zeros_like(x_ref)
    for src in range(16):
        total += buf[(me + 16 - src) % 16]
    o_ref[...] = total


def _allsum(block):
    return pl.pallas_call(
        _allsum_body,
        out_shape=jax.ShapeDtypeStruct((8, LANES), f32),
        in_specs=[pl.BlockSpec(memory_space=pltpu.VMEM)],
        out_specs=pl.BlockSpec(memory_space=pltpu.VMEM),
        scratch_shapes=[
            pltpu.VMEM((16, 8, LANES), f32),
            pltpu.SemaphoreType.DMA((16,)),
            pltpu.SemaphoreType.DMA((16,)),
        ],
        compiler_params=pltpu.CompilerParams(collective_id=0, has_side_effects=True),
        name="allsum",
    )(block)


def _adam_body(c_ref, *refs):
    g_refs = refs[:L]
    w_ref, m_ref, v_ref = refs[L:L + 3]
    wn_ref, mn_ref, vn_ref, wb_ref = refs[-4:]
    c = c_ref[0]
    for l in range(L):
        scaled = c * g_refs[l][...]
        m_new = ADAM_BETA1 * m_ref[l] + (1.0 - ADAM_BETA1) * scaled
        v_new = ADAM_BETA2 * v_ref[l] + (1.0 - ADAM_BETA2) * scaled * scaled
        m_hat = m_new / (1.0 - ADAM_BETA1**ADAM_STEP)
        v_hat = v_new / (1.0 - ADAM_BETA2**ADAM_STEP)
        w = w_ref[l]
        w_new = w - LEARN_RATE * (m_hat / (jnp.sqrt(v_hat) + ADAM_EPS) + WEIGHT_DECAY * w)
        mn_ref[l] = m_new
        vn_ref[l] = v_new
        wn_ref[l] = w_new
        wb_ref[l] = w_new.astype(bf16)


def _adam_chunk(k, c, grads, w, m, v, prev):
    bq = CHUNK_Q // 4
    first = k * (CHUNK_Q // bq)
    state = jax.ShapeDtypeStruct((L, SHARD_Q, LANES), f32)
    spec = pl.BlockSpec((L, bq, LANES), lambda i: (0, first + i, 0))
    in_specs = [pl.BlockSpec(memory_space=pltpu.SMEM)] + [pl.BlockSpec((bq, LANES), lambda i: (first + i, 0))] * L + [spec] * 3
    args = [c, *grads, w, m, v]
    aliases = {}
    if prev is not None:
        in_specs += [pl.BlockSpec(memory_space=pl.ANY)] * 3
        aliases = {len(args) + i: i for i in range(3)}
        args += list(prev)
    return pl.pallas_call(
        _adam_body,
        grid=(CHUNK_Q // bq,),
        out_shape=[state, state, state, jax.ShapeDtypeStruct((L, CHUNK_Q, LANES), bf16)],
        in_specs=in_specs,
        out_specs=[spec, spec, spec, pl.BlockSpec((L, bq, LANES), lambda i: (0, i, 0))],
        input_output_aliases=aliases,
        compiler_params=_params(),
        cost_estimate=_cost(6e9, 30 * L * CHUNK_Q * LANES),
        name="adam",
    )(*args)


def _pack_body(d_ref, *refs, bq):
    parts = refs[:10]
    o_ref, scr = refs[-2:]
    src = pl.program_id(1)
    i = pl.program_id(0)

    def put(read):
        def group(j, carry):
            row = pl.multiple_of(j * 16, 16)
            for l in range(L):
                v = read(l, row).astype(f32)
                scr[pl.ds(l, 16, stride=8), :] = v
            for q in range(16):
                base = pl.multiple_of(j * (16 * LANES) + q * LANES, LANES)
                o_ref[0, :, pl.ds(base, LANES)] = scr[q * 8:q * 8 + L, :].astype(bf16)
            return carry

        lax.fori_loop(0, bq // 16, group, 0)

    for n in range(6):

        @pl.when(src == n)
        def _(n=n):
            put(lambda l, row: parts[n][l, pl.ds(row, 16), :])

    for n in range(2):

        @pl.when((src == 6 + n) & (i == 0))
        def _(n=n):
            put(lambda l, row: parts[6 + 2 * n][l, pl.ds(row, 16), :])

        @pl.when((src == 6 + n) & (i == 1))
        def _(n=n):
            put(lambda l, row: parts[7 + 2 * n][l, pl.ds(row, 16), :])


def _pack_chunk(k, device, parts, prev):
    bq = CHUNK_Q // 2
    flips = (0, 2, 4, 1, 3, 5, 6, 7)

    def out_map(i, src, d_ref):
        flip = jnp.int32(flips[0])
        for n in range(1, 8):
            flip = jnp.where(src == n, flips[n], flip)
        return (0, 0, ((d_ref[0] ^ flip) * CHUNKS + k) * 2 + i)

    in_specs = [pl.BlockSpec((L, bq, LANES), lambda i, src, d_ref: (0, i, 0))] * 6 + [
        pl.BlockSpec((L, bq, LANES), lambda i, src, d_ref: (0, 0, 0))
    ] * 4
    args = [device, *parts]
    aliases = {}
    if prev is not None:
        in_specs += [pl.BlockSpec(memory_space=pl.ANY)]
        aliases = {len(args): 0}
        args += [prev]
    return pl.pallas_call(
        functools.partial(_pack_body, bq=bq),
        grid_spec=pltpu.PrefetchScalarGridSpec(
            num_scalar_prefetch=1,
            grid=(2, 8),
            in_specs=in_specs,
            out_specs=pl.BlockSpec((1, L, bq * LANES), out_map),
            scratch_shapes=[pltpu.VMEM((LANES, LANES), f32)],
        ),
        out_shape=jax.ShapeDtypeStruct((1, L, 8 * SHARD_Q * LANES), bf16),
        input_output_aliases=aliases,
        compiler_params=_params(),
        cost_estimate=_cost(8e9, 4 * 8 * L * CHUNK_Q * LANES),
        name="pack",
    )(*args)


def _flip(a, mask):
    return lax.ppermute(a, "data", [(d, d ^ mask) for d in range(8)])


def solution(mesh):
    def device_step(x_in, targets, w_work, w_master, m_prior, v_prior, clip_tau):
        stage = lax.axis_index("stage")
        first = stage == 0
        device = lax.axis_index("data").astype(jnp.int32).reshape(1)
        x0 = x_in.reshape(ROWS, D)
        w1 = _unpack(w_work, D, F, 32, True)
        w2 = _unpack(w_work, F, D, 128, False)

        (h_first,) = _forward(x0, w1, w2, False)
        act = lax.ppermute(h_first, "stage", [(0, 1)])
        xs, us, h_last = _forward(jnp.where(first, x0, act), w1, w2, True)
        residual = h_last.astype(f32) - targets.reshape(ROWS, D).astype(f32)
        loss_local = jnp.where(first, 0.0, 0.5 * jnp.sum(residual * residual))
        g_top = (residual / TOTAL_ROWS).astype(bf16)
        g_mid = _backward_all(g_top, us, w1, w2)
        g = jnp.where(first, lax.ppermute(g_mid, "stage", [(1, 0)]), g_top)

        grads = [None] * L
        sq_local = jnp.zeros((), f32)
        for layer in reversed(range(L)):
            along_x = layer % 2 == 1
            mask, other = (2, 4) if along_x else (4, 2)
            xf = _flip(xs[layer:layer + 1], mask)
            gf = _flip(g, mask)
            du, g_next = _backward_layer(layer, g, us, w1, w2)
            keep, send = _wgrad(layer, xs, xf, g, gf, us, du, w1, w2, along_x)
            recv = _flip(send, 1)
            far = _flip(keep[1] + recv[1], other)
            grads[layer] = keep[0] + recv[0] + far
            sq_local = sq_local + jnp.sum(grads[layer] * grads[layer])
            g = g_next

        row = lax.broadcasted_iota(jnp.int32, (8, LANES), 0)
        sums = _allsum(jnp.where(row == 0, sq_local, loss_local))
        clip_scale = jnp.minimum(1.0, clip_tau / jnp.sqrt(sums[0, 0]))
        loss_mean = sums[1, 0] / TOTAL_ROWS

        c = clip_scale.reshape(1)
        w, m, v = (a.reshape(L, SHARD_Q, LANES) for a in (w_master, m_prior, v_prior))
        prev = None
        gathered = []
        for k in range(CHUNKS):
            *prev, wb = _adam_chunk(k, c, grads, w, m, v, prev)
            from_x = _flip(wb, 2)
            from_y = _flip(wb, 4)
            half = CHUNK_Q // 2
            diag = (_flip(from_x[:, :half], 4), _flip(from_y[:, half:], 2))
            own = (wb, from_x, from_y)
            gathered.append(own + tuple(_flip(a, 1) for a in own) + diag + tuple(_flip(a, 1) for a in diag))
        w_bf16 = None
        for k in range(CHUNKS):
            w_bf16 = _pack_chunk(k, device, gathered[k], w_bf16)
        shard = (1, L, SHARD_Q * LANES)
        return loss_mean, w_bf16, *(a.reshape(shard) for a in prev)

    row_spec = P(None, "data", None)
    shard_spec = P("stage", None, "data")
    stage_spec = P("stage", None, None)
    return jax.shard_map(
        device_step,
        mesh=mesh,
        in_specs=(row_spec, row_spec, stage_spec, shard_spec, shard_spec, shard_spec, P()),
        out_specs=(P(), stage_spec, shard_spec, shard_spec, shard_spec),
        check_vma=False,
    )
```
